32 devices in a mesh: dp: 4 (over y, z), tp: 8 (over x, core).
Axes of the slice: x: 4, y: 2, z: 2, core: 2. Of those that a mesh axis runs over, the one named last changes fastest.
The devices are a block of a 4x4x8 slice.
Arguments:
- hidden: bfloat16 [8, 64, 2048], P('dp', None, 'tp'), parts along dimension 0
- ln_scale: float32 [2048], P('tp')
- w_head: bfloat16 [2048, 256384], P(None, 'tp')
- targets: int32 [8, 64], P('dp'), parts along dimension 0
- valid_mask: int32 [8, 64], P('dp'), parts along dimension 0
Outputs:
- output 1: float32 [8, 64], P('dp'), parts along dimension 0
- output 2: float32 [8], P('dp'), parts along dimension 0
There are 4 independent parts. The reference program is written for one: setup_inputs(seed, part) draws one part's arguments, and reference() takes and returns one part's arrays. A program takes and returns all parts, laid end to end along the dimension named above; an argument that names none is the same for every part.
All inputs are finite; a program needn't handle non-finite values.
Results may differ from the reference program's by a relative error of at most 0.001.
Values are sent between devices in bfloat16 or wider.
A program may use at most 768 MiB of HBM per device.

```python
import math
import jax
import jax.numpy as jnp
from jax import lax

D = 2048
VOCAB_SIZE = 256384
SEQ_COUNT = 2
SEQ_LEN = 64
REGIONS = 16
ROW_BLOCK = 32

NORM_EPS = 1e-6


def setup_inputs(seed: int = 0, part: int = 0) -> dict:
    base_key = jax.random.key(seed)
    key_head, key_scale = jax.random.split(base_key, 2)
    part_key = jax.random.fold_in(base_key, part)
    key_noise, key_gain, key_boost, key_route = jax.random.split(part_key, 4)
    key_tgt, key_len, key_pick = jax.random.split(key_route, 3)
    tokens = SEQ_COUNT * SEQ_LEN
    w_f32 = jax.random.normal(key_head, (D, VOCAB_SIZE), jnp.float32) * (2.0 / math.sqrt(D))
    w_head = w_f32.astype(jnp.bfloat16)
    ln_scale = jax.random.uniform(key_scale, (D,), jnp.float32, 0.5, 1.5)
    target_ids = jax.random.randint(key_tgt, (SEQ_COUNT, SEQ_LEN), 0, VOCAB_SIZE, jnp.int32)
    target_ids = target_ids.at[0, 0].set(VOCAB_SIZE - 1).at[0, 1].set(0)
    lengths = jax.random.randint(key_len, (SEQ_COUNT,), 1, SEQ_LEN, jnp.int32)
    full_pick = jax.random.randint(key_pick, (), 0, SEQ_COUNT, jnp.int32)
    lengths = jnp.where(jnp.arange(SEQ_COUNT) == full_pick, SEQ_LEN, lengths)
    valid_mask = (jnp.arange(SEQ_LEN)[None, :] < lengths[:, None]).astype(jnp.int32)
    noise_f32 = jax.random.normal(key_noise, (SEQ_COUNT, SEQ_LEN, D), jnp.float32)
    region_gain = jnp.exp(0.8 * jax.random.normal(key_gain, (SEQ_COUNT, SEQ_LEN, REGIONS), jnp.float32))
    base_rows = noise_f32 * jnp.repeat(region_gain, D // REGIONS, axis=2)
    base_rms = jnp.sqrt(jnp.mean(base_rows * base_rows, axis=-1, keepdims=True))
    boost_amt = jax.random.uniform(key_boost, (SEQ_COUNT, SEQ_LEN, 1), jnp.float32, 0.0, 6.0)
    target_cols = jnp.take(w_head, target_ids.reshape(tokens), axis=1).T.reshape(SEQ_COUNT, SEQ_LEN, D)
    hidden = (base_rows + boost_amt * base_rms * target_cols.astype(jnp.float32)).astype(jnp.bfloat16)
    return {"hidden": hidden, "ln_scale": ln_scale, "w_head": w_head, "targets": target_ids, "valid_mask": valid_mask}


def reference(hidden, ln_scale, w_head, targets, valid_mask):
    tokens = SEQ_COUNT * SEQ_LEN
    row_blocks = hidden.reshape(tokens // ROW_BLOCK, ROW_BLOCK, D)
    tgt_blocks = targets.reshape(tokens // ROW_BLOCK, ROW_BLOCK)

    def score_block(block_args):
        row_blk, tgt_blk = block_args
        row_f32 = row_blk.astype(jnp.float32)
        inv_rms = lax.rsqrt(jnp.mean(row_f32 * row_f32, axis=-1, keepdims=True) + NORM_EPS)
        normed = (row_f32 * inv_rms * ln_scale).astype(jnp.bfloat16)
        logits = jnp.dot(normed, w_head, preferred_element_type=jnp.float32)
        row_max = jnp.max(logits, axis=-1, keepdims=True)
        log_norm = row_max[:, 0] + jnp.log(jnp.sum(jnp.exp(logits - row_max), axis=-1))
        picked = jnp.take_along_axis(logits, tgt_blk[:, None], axis=1)[:, 0]
        return picked - log_norm

    tok_all = lax.map(score_block, (row_blocks, tgt_blocks)).reshape(SEQ_COUNT, SEQ_LEN)
    token_logp = valid_mask.astype(jnp.float32) * tok_all
    seq_logp = jnp.sum(token_logp, axis=1)
    return (token_logp, seq_logp)
```

```python
import functools

import jax
import jax.numpy as jnp
from jax import lax
from jax.experimental import pallas as pl
from jax.experimental.pallas import tpu as pltpu
from jax.sharding import PartitionSpec as P

NORM_EPS = 1e-6
TILE = 1024
LANES = 128
CHUNK = 128
STRIP = 32
SLOTS = 13
UNROLL = 4
PAIR = True
MESH = pl.DeviceIdType.MESH
NEG_INF = float("-inf")


def plan(v_local, pair):
    sides = 2 if pair else 1
    half = -(-v_local // (16 * sides)) * 16
    return half, half // TILE, half % TILE


def kernel(cfg, h_hbm, g_hbm, w_hbm, tgt_hbm, out_ref,
           hb, gb, tg, xb, qb, wb, wt, za, zb, st, sbuf,
           loc_sem, w_sem, t_sem, snd, rcv, g_snd, g_rcv, f_snd, f_rcv):
    tp, pair, v_local = cfg
    groups = 2 if pair else 1
    rows, feat = h_hbm.shape
    seqs, slen = tgt_hbm.shape
    half, n_full, tail = plan(v_local, pair)
    nx = tp // 2
    me_dp = lax.axis_index("dp")
    me = lax.axis_index("tp")
    x, core = me // 2, me % 2
    side = me_dp % 2 if pair else 0
    mate_dp = me_dp + 1 - 2 * (me_dp % 2) if pair else me_dp
    right = 2 * ((x + 1) % nx) + core
    left = 2 * ((x + nx - 1) % nx) + core
    far = 2 * ((x + 2) % nx) + core
    flip = 1 - 2 * core
    other = me + flip
    row0 = side * (v_local - half)

    h_cp = pltpu.make_async_copy(h_hbm, hb.at[0, me], loc_sem.at[0])
    g_cp = pltpu.make_async_copy(g_hbm, gb.at[me], loc_sem.at[1])
    t_in = pltpu.make_async_copy(tgt_hbm, tg.at[0], loc_sem.at[2])
    for cp in (h_cp, g_cp, t_in):
        cp.start()

    def w_copy(i):
        slot = i % SLOTS if isinstance(i, int) else lax.rem(i, SLOTS)
        start = row0 + i * TILE
        return pltpu.make_async_copy(
            w_hbm.at[pl.ds(pl.multiple_of(start, 16), TILE), :], wb.at[slot], w_sem.at[slot])

    tail_cp = pltpu.make_async_copy(
        w_hbm.at[pl.ds(pl.multiple_of(row0 + n_full * TILE, 16), tail), :], wt, t_sem.at[0])
    def fetch(first, stop):
        for i in range(first, min(stop, n_full)):
            w_copy(i).start()

    fetch(0, 1)

    to_right, to_left, to_other, to_mate = (me_dp, right), (me_dp, left), (me_dp, other), (mate_dp, me)
    near = [to_right, to_left, to_other]
    mate_right, mate_left = (mate_dp, right), (mate_dp, left)
    if pair:
        near += [to_mate, mate_right, mate_left]
    barrier = pltpu.get_barrier_semaphore()
    for dev in near:
        pl.semaphore_signal(barrier, inc=1, device_id=dev, device_id_type=MESH)
    h_cp.wait()
    g_cp.wait()
    t_in.wait()
    pl.semaphore_wait(barrier, len(near))

    started = []

    def remote(src, dst, s_sem, r_sem, dev):
        return pltpu.make_async_remote_copy(
            src_ref=src, dst_ref=dst, send_sem=s_sem, recv_sem=r_sem, device_id=dev, device_id_type=MESH)

    def send(grp, origin, part, flow, dev, grp_dst):
        cp = remote(hb.at[grp, origin, part], hb.at[grp_dst, origin, part], snd.at[flow], rcv.at[flow], dev)
        cp.start()
        started.append(cp)

    def arrived(grp, origin, part, flow):
        ref = hb.at[grp, origin, part]
        remote(ref, ref, snd.at[flow], rcv.at[flow], to_other).wait_recv()

    def g_send(origin, flow, dev):
        cp = remote(gb.at[origin], gb.at[origin], g_snd.at[flow], g_rcv.at[flow], dev)
        cp.start()
        started.append(cp)

    def g_arrived(origin, flow):
        remote(gb.at[origin], gb.at[origin], g_snd.at[flow], g_rcv.at[flow], to_other).wait_recv()

    RING, SIDE, MATE, MSIDE = 0, 8, 16, 24
    lo, hi, both = pl.ds(0, rows // 2), pl.ds(rows // 2, rows // 2), pl.ds(0, rows)
    lane = [me, left, right, far]

    def both_groups(part, flow, own_dev, mate_dev):
        send(0, me, part, RING + flow, own_dev, 0)
        if pair:
            send(0, me, part, MATE + flow, mate_dev, 1)

    both_groups(lo, 0, to_right, mate_right)
    both_groups(hi, 1, to_left, mate_left)
    both_groups(hi, 2, to_right, mate_right)
    both_groups(lo, 3, to_left, mate_left)
    if pair:
        send(0, me, both, MATE + 6, to_mate, 1)
    send(0, me, both, SIDE + 0, to_other, 0)
    g_send(me, 0, to_right)
    g_send(me, 1, to_left)
    g_send(me, 3, to_other)
    if pair:
        t_cp = remote(tg.at[0], tg.at[1], g_snd.at[7], g_rcv.at[7], to_mate)
        t_cp.start()
        started.append(t_cp)
    fetch(1, 3)
    flows = ((0, RING, SIDE), (1, MATE, MSIDE))[:groups]
    for grp, ring, _ in flows:
        arrived(grp, left, lo, ring + 0)
        send(grp, left, lo, ring + 4, to_right, grp)
        arrived(grp, right, hi, ring + 1)
        send(grp, right, hi, ring + 5, to_left, grp)
    fetch(3, 5)
    g_arrived(left, 0)
    g_send(left, 2, to_right)
    g_send(left, 4, to_other)
    g_arrived(right, 1)
    g_send(right, 5, to_other)
    if pair:
        arrived(1, me, both, MATE + 6)
        send(1, me, both, MSIDE + 0, to_other, 1)
    for grp, ring, across in flows:
        arrived(grp, left, hi, ring + 2)
        send(grp, left, both, across + 1, to_other, grp)
        arrived(grp, right, lo, ring + 3)
        send(grp, right, both, across + 2, to_other, grp)
    fetch(5, 7)
    g_arrived(far, 2)
    g_send(far, 6, to_other)
    for grp, ring, across in flows:
        arrived(grp, far, lo, ring + 4)
        arrived(grp, far, hi, ring + 5)
        send(grp, far, both, across + 3, to_other, grp)
    fetch(7, SLOTS)
    for k in range(4):
        arrived(0, lane[k] + flip, both, SIDE + k)
    for k, origin in ((3, me), (4, left), (5, right), (6, far)):
        g_arrived(origin + flip, k)

    def squares(grp, blocks, fresh_sum):
        for r in range(0, rows, STRIP):
            acc = jnp.zeros((STRIP, LANES), jnp.float32) if fresh_sum else qb[r:r + STRIP, :]
            for j in blocks:
                v = hb[grp, j, r:r + STRIP, :].astype(jnp.float32)
                sq = v * v
                for c in range(0, feat, LANES):
                    acc += sq[:, c:c + LANES]
            qb[r:r + STRIP, :] = acc

    def normalize(grp):
        for r in range(0, rows, STRIP):
            total = jnp.sum(qb[r:r + STRIP, :], axis=1, keepdims=True)
            inv = lax.rsqrt(total / (feat * tp) + NORM_EPS)
            for j in range(tp):
                v = hb[grp, j, r:r + STRIP, :].astype(jnp.float32)
                xb[grp * rows + r:grp * rows + r + STRIP, j * feat:(j + 1) * feat] = (
                    v * inv * gb[j]).astype(jnp.bfloat16)

    def places_of(grp):
        ids = jnp.concatenate([tg[grp, b:b + 1, :] for b in range(seqs)], axis=1)
        return jnp.broadcast_to(ids - me * v_local, (8, rows)) - lax.broadcasted_iota(jnp.int32, (8, rows), 0)

    def fresh():
        return (jnp.full((8, rows), NEG_INF, jnp.float32), jnp.zeros((8, rows), jnp.float32),
                jnp.zeros((8, rows), jnp.float32))

    def dot(z_ref, w_rows, n, cols=groups * rows):
        cut = -(-n // 32) * 16
        for r0, r1 in ((0, cut), (cut, n)):
            z_ref[r0:r1, 0:cols] = lax.dot_general(
                w_rows(r0, r1), xb[0:cols, :], (((1,), (1,)), ((), ())), preferred_element_type=jnp.float32)

    def tile_rows(slot):
        return lambda r0, r1: wb[slot, r0:r1, :]

    def absorb(z_ref, base, n, state, places, first_masked=None):
        m, s, t = state
        for r in range(0, n, CHUNK):
            zs, hits = [], []
            for q in range(r, min(r + CHUNK, n), 8):
                z = z_ref[q:q + 8, 0:m.shape[1]]
                hit = places == base + q
                if first_masked is not None and q >= first_masked:
                    z = jnp.where(side > 0, z, NEG_INF)
                    hit = hit & (side > 0)
                zs.append(z)
                hits.append(hit)
            tree = list(zs)
            while len(tree) > 1:
                tree = [jnp.maximum(*tree[i:i + 2]) if i + 1 < len(tree) else tree[i]
                        for i in range(0, len(tree), 2)]
            top = jnp.maximum(m, tree[0])
            es = [jnp.exp(z - top) for z in zs]
            while len(es) > 1:
                es = [es[i] + es[i + 1] if i + 1 < len(es) else es[i] for i in range(0, len(es), 2)]
            s = s * jnp.exp(m - top) + es[0]
            for z, hit in zip(zs, hits):
                t = jnp.where(hit, z, t)
            m = top
        return m, s, t

    squares(0, range(tp), True)
    normalize(0)
    own_places, state = places_of(0), fresh()
    if pair:
        for k in range(3):
            arrived(1, lane[k] + flip, both, MSIDE + k)
        squares(1, [j for k in range(3) for j in (lane[k], lane[k] + flip)], True)
        arrived(1, far + flip, both, MSIDE + 3)
        squares(1, (far, far + flip), False)
        t_cp.wait_recv()
        normalize(1)
        places = jnp.concatenate([own_places, places_of(1)], axis=1)
        state = tuple(jnp.concatenate(p, axis=1) for p in zip(state, fresh()))
    else:
        places = own_places

    bufs = (za, zb)

    def refill(i):
        if 0 <= i - 1 < n_full - SLOTS:
            w_copy(i - 1 + SLOTS).start()
            if i + SLOTS == n_full:
                tail_cp.start()

    def run(first, count, state):
        for q in range(count):
            i = first + q
            nxt = (i + 1) % SLOTS if isinstance(i, int) else lax.rem(i + 1, SLOTS)
            dot(bufs[(q + 1) % 2], tile_rows(nxt), TILE)
            state = absorb(bufs[q % 2], row0 + i * TILE, TILE, state, places)
        return state

    trips, rest = divmod(n_full - 1, UNROLL)
    if rest % 2 or UNROLL % 2 or n_full != SLOTS + rest:
        raise ValueError("tile count")
    for i in range(rest + 1):
        w_copy(i).wait()
    dot(za, tile_rows(0), TILE)
    state = run(0, rest, state)
    for i in range(1, rest + 1):
        refill(i)

    def trip(j, state):
        first = rest + UNROLL * j
        for q in range(UNROLL):
            w_copy(first + q + 1).wait()
        return run(first, UNROLL, state)

    state = lax.fori_loop(0, trips, trip, state)
    tail_cp.wait()
    dot(bufs[1], lambda r0, r1: wt[r0:r1, :], tail)
    state = absorb(bufs[0], row0 + (n_full - 1) * TILE, TILE, state, places)
    twice = groups * half - v_local
    m, s, t = absorb(bufs[1], row0 + n_full * TILE, tail, state, places, tail - twice if twice else None)

    top = jnp.max(m, axis=0, keepdims=True)
    total = jnp.sum(s * jnp.exp(m - top), axis=0, keepdims=True)
    picked = jnp.sum(t, axis=0, keepdims=True)
    for grp in range(groups):
        gs = slice(grp * rows, (grp + 1) * rows)
        st[grp] = jnp.concatenate(
            [top[:, gs], total[:, gs], picked[:, gs], jnp.zeros((5, rows), jnp.float32)], axis=0)

    if pair:
        for k in range(tp):
            cp = remote(st.at[1], sbuf.at[1, me], f_snd.at[tp + k], f_rcv.at[tp + k], (mate_dp, (me + k) % tp))
            cp.start()
            started.append(cp)
    for k in range(1, tp):
        cp = remote(st.at[0], sbuf.at[0, me], f_snd.at[k], f_rcv.at[k], (me_dp, (me + k) % tp))
        cp.start()
        started.append(cp)
    sbuf[0, me] = st[0]
    for k in range(1, tp):
        ref = sbuf.at[0, (me + tp - k) % tp]
        remote(ref, ref, f_snd.at[k], f_rcv.at[k], to_other).wait_recv()
    if pair:
        for k in range(tp):
            ref = sbuf.at[1, (me + tp - k) % tp]
            remote(ref, ref, f_snd.at[tp + k], f_rcv.at[tp + k], to_other).wait_recv()

    parts = [sbuf[g, j] for g in range(groups) for j in range(tp)]
    top = functools.reduce(jnp.maximum, parts)[0:1, :]
    total = functools.reduce(jnp.add, [p[1:2, :] * jnp.exp(p[0:1, :] - top) for p in parts])
    picked = functools.reduce(jnp.add, parts)[2:3, :]
    logp = picked - (top + jnp.log(total))
    for b in range(seqs):
        out_ref[b:b + 1, :] = logp[:, b * slen:(b + 1) * slen]
    for cp in started:
        cp.wait_send()


def solution(mesh):
    tp = mesh.shape["tp"]
    pair = PAIR and mesh.shape["dp"] % 2 == 0

    def local_score(hidden, ln_scale, w_head, targets, valid_mask):
        seqs, slen, feat = hidden.shape
        rows, d, v_local = seqs * slen, w_head.shape[0], w_head.shape[1]
        groups = 2 if pair else 1
        tail = plan(v_local, pair)[2]
        f32, bf16 = jnp.float32, jnp.bfloat16
        dma = pltpu.SemaphoreType.DMA
        logp = pl.pallas_call(
            functools.partial(kernel, (tp, pair, v_local)),
            out_shape=jax.ShapeDtypeStruct((seqs, slen), f32),
            in_specs=[pl.BlockSpec(memory_space=pl.ANY)] * 4,
            out_specs=pl.BlockSpec(memory_space=pltpu.VMEM),
            scratch_shapes=[
                pltpu.VMEM((groups, tp, rows, feat), bf16),
                pltpu.VMEM((tp, 1, feat), f32),
                pltpu.VMEM((2, seqs, slen), jnp.int32),
                pltpu.VMEM((groups * rows, d), bf16),
                pltpu.VMEM((rows, LANES), f32),
                pltpu.VMEM((SLOTS, TILE, d), bf16),
                pltpu.VMEM((tail, d), bf16),
                pltpu.VMEM((TILE, groups * rows), f32),
                pltpu.VMEM((TILE, groups * rows), f32),
                pltpu.VMEM((groups, 8, rows), f32),
                pltpu.VMEM((groups, tp, 8, rows), f32),
                dma((3,)), dma((SLOTS,)), dma((1,)),
                dma((32,)), dma((32,)), dma((8,)), dma((8,)), dma((2 * tp,)), dma((2 * tp,)),
            ],
            compiler_params=pltpu.CompilerParams(
                collective_id=0, has_side_effects=True, vmem_limit_bytes=67043328),
            name="score",
        )(hidden.reshape(rows, feat), ln_scale.reshape(1, feat), w_head.T, targets)
        token_logp = valid_mask.astype(f32) * logp
        return token_logp, jnp.sum(token_logp, axis=1)

    return jax.shard_map(
        local_score,
        mesh=mesh,
        in_specs=(P("dp", None, "tp"), P("tp"), P(None, "tp"), P("dp", None), P("dp", None)),
        out_specs=(P("dp", None), P("dp")),
        check_vma=False,
    )
```

```python
import functools

import jax
import jax.numpy as jnp
from jax import lax
from jax.experimental import pallas as pl
from jax.experimental.pallas import tpu as pltpu
from jax.sharding import PartitionSpec as P

NORM_EPS = 1e-6
TILE = 1024
LANES = 128
CHUNK = 128
STRIP = 32
SLOTS = 13
UNROLL = 4
PAIR = True
MESH = pl.DeviceIdType.MESH
NEG_INF = float("-inf")


def plan(v_local, pair):
    sides = 2 if pair else 1
    half = -(-v_local // (16 * sides)) * 16
    return half, half // TILE, half % TILE


def kernel(cfg, h_hbm, g_hbm, w_hbm, tgt_hbm, out_ref,
           hb, gb, tg, xb, qb, wb, wt, za, zb, st, sbuf,
           loc_sem, w_sem, t_sem, snd, rcv, g_snd, g_rcv, f_snd, f_rcv):
    tp, pair, v_local = cfg
    groups = 2 if pair else 1
    rows, feat = h_hbm.shape
    seqs, slen = tgt_hbm.shape
    half, n_full, tail = plan(v_local, pair)
    nx = tp // 2
    me_dp = lax.axis_index("dp")
    me = lax.axis_index("tp")
    x, core = me // 2, me % 2
    side = me_dp % 2 if pair else 0
    mate_dp = me_dp + 1 - 2 * (me_dp % 2) if pair else me_dp
    right = 2 * ((x + 1) % nx) + core
    left = 2 * ((x + nx - 1) % nx) + core
    far = 2 * ((x + 2) % nx) + core
    flip = 1 - 2 * core
    other = me + flip
    row0 = side * (v_local - half)

    h_cp = pltpu.make_async_copy(h_hbm, hb.at[0, me], loc_sem.at[0])
    g_cp = pltpu.make_async_copy(g_hbm, gb.at[me], loc_sem.at[1])
    t_in = pltpu.make_async_copy(tgt_hbm, tg.at[0], loc_sem.at[2])
    h_cp.start()

    def w_copy(i):
        slot = i % SLOTS if isinstance(i, int) else lax.rem(i, SLOTS)
        start = row0 + i * TILE
        return pltpu.make_async_copy(
            w_hbm.at[pl.ds(pl.multiple_of(start, 16), TILE), :], wb.at[slot], w_sem.at[slot])

    tail_cp = pltpu.make_async_copy(
        w_hbm.at[pl.ds(pl.multiple_of(row0 + n_full * TILE, 16), tail), :], wt, t_sem.at[0])
    def fetch(first, stop):
        for i in range(first, min(stop, n_full)):
            w_copy(i).start()

    to_right, to_left, to_other, to_mate = (me_dp, right), (me_dp, left), (me_dp, other), (mate_dp, me)
    near = [to_right, to_left, to_other]
    mate_right, mate_left = (mate_dp, right), (mate_dp, left)
    if pair:
        near += [to_mate, mate_right, mate_left]
    barrier = pltpu.get_barrier_semaphore()
    for dev in near:
        pl.semaphore_signal(barrier, inc=1, device_id=dev, device_id_type=MESH)
    g_cp.start()
    t_in.start()

    fetch(0, 1)
    h_cp.wait()
    g_cp.wait()
    t_in.wait()
    pl.semaphore_wait(barrier, len(near))

    started = []

    def remote(src, dst, s_sem, r_sem, dev):
        return pltpu.make_async_remote_copy(
            src_ref=src, dst_ref=dst, send_sem=s_sem, recv_sem=r_sem, device_id=dev, device_id_type=MESH)

    def send(grp, origin, part, flow, dev, grp_dst):
        cp = remote(hb.at[grp, origin, part], hb.at[grp_dst, origin, part], snd.at[flow], rcv.at[flow], dev)
        cp.start()
        started.append(cp)

    def arrived(grp, origin, part, flow):
        ref = hb.at[grp, origin, part]
        remote(ref, ref, snd.at[flow], rcv.at[flow], to_other).wait_recv()

    def g_send(origin, flow, dev):
        cp = remote(gb.at[origin], gb.at[origin], g_snd.at[flow], g_rcv.at[flow], dev)
        cp.start()
        started.append(cp)

    def g_arrived(origin, flow):
        remote(gb.at[origin], gb.at[origin], g_snd.at[flow], g_rcv.at[flow], to_other).wait_recv()

    RING, SIDE, MATE, MSIDE = 0, 8, 16, 24
    lo, hi, both = pl.ds(0, rows // 2), pl.ds(rows // 2, rows // 2), pl.ds(0, rows)
    lane = [me, left, right, far]

    def both_groups(part, flow, own_dev, mate_dev):
        send(0, me, part, RING + flow, own_dev, 0)
        if pair:
            send(0, me, part, MATE + flow, mate_dev, 1)

    both_groups(lo, 0, to_right, mate_right)
    both_groups(hi, 1, to_left, mate_left)
    both_groups(hi, 2, to_right, mate_right)
    both_groups(lo, 3, to_left, mate_left)
    if pair:
        send(0, me, both, MATE + 6, to_mate, 1)
    send(0, me, both, SIDE + 0, to_other, 0)
    g_send(me, 0, to_right)
    g_send(me, 1, to_left)
    g_send(me, 3, to_other)
    if pair:
        t_cp = remote(tg.at[0], tg.at[1], g_snd.at[7], g_rcv.at[7], to_mate)
        t_cp.start()
        started.append(t_cp)
    fetch(1, 3)
    flows = ((0, RING, SIDE), (1, MATE, MSIDE))[:groups]
    for grp, ring, _ in flows:
        arrived(grp, left, lo, ring + 0)
        send(grp, left, lo, ring + 4, to_right, grp)
        arrived(grp, right, hi, ring + 1)
        send(grp, right, hi, ring + 5, to_left, grp)
    fetch(3, 5)
    g_arrived(left, 0)
    g_send(left, 2, to_right)
    g_send(left, 4, to_other)
    g_arrived(right, 1)
    g_send(right, 5, to_other)
    if pair:
        arrived(1, me, both, MATE + 6)
        send(1, me, both, MSIDE + 0, to_other, 1)
    for grp, ring, across in flows:
        arrived(grp, left, hi, ring + 2)
        send(grp, left, both, across + 1, to_other, grp)
        arrived(grp, right, lo, ring + 3)
        send(grp, right, both, across + 2, to_other, grp)
    fetch(5, 7)
    g_arrived(far, 2)
    g_send(far, 6, to_other)
    for grp, ring, across in flows:
        arrived(grp, far, lo, ring + 4)
        arrived(grp, far, hi, ring + 5)
        send(grp, far, both, across + 3, to_other, grp)
    fetch(7, SLOTS)
    for k in range(4):
        arrived(0, lane[k] + flip, both, SIDE + k)
    for k, origin in ((3, me), (4, left), (5, right), (6, far)):
        g_arrived(origin + flip, k)

    def squares(grp, blocks, fresh_sum):
        for r in range(0, rows, STRIP):
            acc = jnp.zeros((STRIP, LANES), jnp.float32) if fresh_sum else qb[r:r + STRIP, :]
            for j in blocks:
                v = hb[grp, j, r:r + STRIP, :].astype(jnp.float32)
                sq = v * v
                for c in range(0, feat, LANES):
                    acc += sq[:, c:c + LANES]
            qb[r:r + STRIP, :] = acc

    def normalize(grp):
        for r in range(0, rows, STRIP):
            total = jnp.sum(qb[r:r + STRIP, :], axis=1, keepdims=True)
            inv = lax.rsqrt(total / (feat * tp) + NORM_EPS)
            for j in range(tp):
                v = hb[grp, j, r:r + STRIP, :].astype(jnp.float32)
                xb[grp * rows + r:grp * rows + r + STRIP, j * feat:(j + 1) * feat] = (
                    v * inv * gb[j]).astype(jnp.bfloat16)

    def places_of(grp):
        ids = jnp.concatenate([tg[grp, b:b + 1, :] for b in range(seqs)], axis=1)
        return jnp.broadcast_to(ids - me * v_local, (8, rows)) - lax.broadcasted_iota(jnp.int32, (8, rows), 0)

    def fresh():
        return (jnp.full((8, rows), NEG_INF, jnp.float32), jnp.zeros((8, rows), jnp.float32),
                jnp.zeros((8, rows), jnp.float32))

    def dot(z_ref, w_rows, n, cols=groups * rows):
        cut = -(-n // 32) * 16
        for r0, r1 in ((0, cut), (cut, n)):
            z_ref[r0:r1, 0:cols] = lax.dot_general(
                w_rows(r0, r1), xb[0:cols, :], (((1,), (1,)), ((), ())), preferred_element_type=jnp.float32)

    def tile_rows(slot):
        return lambda r0, r1: wb[slot, r0:r1, :]

    def absorb(z_ref, base, n, state, places, first_masked=None):
        m, s, t = state
        for r in range(0, n, CHUNK):
            zs, hits = [], []
            for q in range(r, min(r + CHUNK, n), 8):
                z = z_ref[q:q + 8, 0:m.shape[1]]
                hit = places == base + q
                if first_masked is not None and q >= first_masked:
                    z = jnp.where(side > 0, z, NEG_INF)
                    hit = hit & (side > 0)
                zs.append(z)
                hits.append(hit)
            tree = list(zs)
            while len(tree) > 1:
                tree = [jnp.maximum(*tree[i:i + 2]) if i + 1 < len(tree) else tree[i]
                        for i in range(0, len(tree), 2)]
            top = jnp.maximum(m, tree[0])
            es = [jnp.exp(z - top) for z in zs]
            while len(es) > 1:
                es = [es[i] + es[i + 1] if i + 1 < len(es) else es[i] for i in range(0, len(es), 2)]
            s = s * jnp.exp(m - top) + es[0]
            for z, hit in zip(zs, hits):
                t = jnp.where(hit, z, t)
            m = top
        return m, s, t

    squares(0, range(tp), True)
    normalize(0)
    own_places, state = places_of(0), fresh()
    if pair:
        for k in range(3):
            arrived(1, lane[k] + flip, both, MSIDE + k)
        squares(1, [j for k in range(3) for j in (lane[k], lane[k] + flip)], True)
        arrived(1, far + flip, both, MSIDE + 3)
        squares(1, (far, far + flip), False)
        t_cp.wait_recv()
        normalize(1)
        places = jnp.concatenate([own_places, places_of(1)], axis=1)
        state = tuple(jnp.concatenate(p, axis=1) for p in zip(state, fresh()))
    else:
        places = own_places

    bufs = (za, zb)

    def refill(i):
        if 0 <= i - 1 < n_full - SLOTS:
            w_copy(i - 1 + SLOTS).start()
            if i + SLOTS == n_full:
                tail_cp.start()

    def run(first, count, state):
        for q in range(count):
            i = first + q
            nxt = (i + 1) % SLOTS if isinstance(i, int) else lax.rem(i + 1, SLOTS)
            dot(bufs[(q + 1) % 2], tile_rows(nxt), TILE)
            state = absorb(bufs[q % 2], row0 + i * TILE, TILE, state, places)
        return state

    trips, rest = divmod(n_full - 1, UNROLL)
    if rest % 2 or UNROLL % 2 or n_full != SLOTS + rest:
        raise ValueError("tile count")
    for i in range(rest + 1):
        w_copy(i).wait()
    dot(za, tile_rows(0), TILE)
    state = run(0, rest, state)
    for i in range(1, rest + 1):
        refill(i)

    def trip(j, state):
        first = rest + UNROLL * j
        for q in range(UNROLL):
            w_copy(first + q + 1).wait()
        return run(first, UNROLL, state)

    state = lax.fori_loop(0, trips, trip, state)
    tail_cp.wait()
    dot(bufs[1], lambda r0, r1: wt[r0:r1, :], tail)
    state = absorb(bufs[0], row0 + (n_full - 1) * TILE, TILE, state, places)
    twice = groups * half - v_local
    m, s, t = absorb(bufs[1], row0 + n_full * TILE, tail, state, places, tail - twice if twice else None)

    top = jnp.max(m, axis=0, keepdims=True)
    total = jnp.sum(s * jnp.exp(m - top), axis=0, keepdims=True)
    picked = jnp.sum(t, axis=0, keepdims=True)
    for grp in range(groups):
        gs = slice(grp * rows, (grp + 1) * rows)
        st[grp] = jnp.concatenate(
            [top[:, gs], total[:, gs], picked[:, gs], jnp.zeros((5, rows), jnp.float32)], axis=0)

    if pair:
        for k in range(tp):
            cp = remote(st.at[1], sbuf.at[1, me], f_snd.at[tp + k], f_rcv.at[tp + k], (mate_dp, (me + k) % tp))
            cp.start()
            started.append(cp)
    for k in range(1, tp):
        cp = remote(st.at[0], sbuf.at[0, me], f_snd.at[k], f_rcv.at[k], (me_dp, (me + k) % tp))
        cp.start()
        started.append(cp)
    sbuf[0, me] = st[0]
    for cp in started:
        cp.wait_send()
    for k in range(1, tp):
        ref = sbuf.at[0, (me + tp - k) % tp]
        remote(ref, ref, f_snd.at[k], f_rcv.at[k], to_other).wait_recv()
    if pair:
        for k in range(tp):
            ref = sbuf.at[1, (me + tp - k) % tp]
            remote(ref, ref, f_snd.at[tp + k], f_rcv.at[tp + k], to_other).wait_recv()

    parts = [sbuf[g, j] for g in range(groups) for j in range(tp)]
    top = functools.reduce(jnp.maximum, parts)[0:1, :]
    total = functools.reduce(jnp.add, [p[1:2, :] * jnp.exp(p[0:1, :] - top) for p in parts])
    picked = functools.reduce(jnp.add, parts)[2:3, :]
    logp = picked - (top + jnp.log(total))
    for b in range(seqs):
        out_ref[b:b + 1, :] = logp[:, b * slen:(b + 1) * slen]


def solution(mesh):
    tp = mesh.shape["tp"]
    pair = PAIR and mesh.shape["dp"] % 2 == 0

    def local_score(hidden, ln_scale, w_head, targets, valid_mask):
        seqs, slen, feat = hidden.shape
        rows, d, v_local = seqs * slen, w_head.shape[0], w_head.shape[1]
        groups = 2 if pair else 1
        tail = plan(v_local, pair)[2]
        f32, bf16 = jnp.float32, jnp.bfloat16
        dma = pltpu.SemaphoreType.DMA
        logp = pl.pallas_call(
            functools.partial(kernel, (tp, pair, v_local)),
            out_shape=jax.ShapeDtypeStruct((seqs, slen), f32),
            in_specs=[pl.BlockSpec(memory_space=pl.ANY)] * 4,
            out_specs=pl.BlockSpec(memory_space=pltpu.VMEM),
            scratch_shapes=[
                pltpu.VMEM((groups, tp, rows, feat), bf16),
                pltpu.VMEM((tp, 1, feat), f32),
                pltpu.VMEM((2, seqs, slen), jnp.int32),
                pltpu.VMEM((groups * rows, d), bf16),
                pltpu.VMEM((rows, LANES), f32),
                pltpu.VMEM((SLOTS, TILE, d), bf16),
                pltpu.VMEM((tail, d), bf16),
                pltpu.VMEM((TILE, groups * rows), f32),
                pltpu.VMEM((TILE, groups * rows), f32),
                pltpu.VMEM((groups, 8, rows), f32),
                pltpu.VMEM((groups, tp, 8, rows), f32),
                dma((3,)), dma((SLOTS,)), dma((1,)),
                dma((32,)), dma((32,)), dma((8,)), dma((8,)), dma((2 * tp,)), dma((2 * tp,)),
            ],
            compiler_params=pltpu.CompilerParams(
                collective_id=0, has_side_effects=True, vmem_limit_bytes=67043328),
            name="score",
        )(hidden.reshape(rows, feat), ln_scale.reshape(1, feat), w_head.T, targets)
        token_logp = valid_mask.astype(f32) * logp
        return token_logp, jnp.sum(token_logp, axis=1)

    return jax.shard_map(
        local_score,
        mesh=mesh,
        in_specs=(P("dp", None, "tp"), P("tp"), P(None, "tp"), P("dp", None), P("dp", None)),
        out_specs=(P("dp", None), P("dp")),
        check_vma=False,
    )
```
